32 devices in a mesh: dp: 2 (over x), sp: 4 (over z), tp: 4 (over y, core).
Axes of the slice: x: 2, y: 2, z: 4, core: 2. Of those that a mesh axis runs over, the one named last changes fastest.
Arguments:
- hidden: bfloat16 [128, 4096], P('dp'), parts along dimension 0
- new_pos: int32 [128], P('dp'), parts along dimension 0
- k_self: bfloat16 [128, 256, 8, 128], P('dp', 'sp', 'tp'), parts along dimension 0
- v_self: bfloat16 [128, 256, 8, 128], P('dp', 'sp', 'tp'), parts along dimension 0
- k_cross: bfloat16 [128, 256, 8, 128], P('dp', None, 'tp'), parts along dimension 0
- v_cross: bfloat16 [128, 256, 8, 128], P('dp', None, 'tp'), parts along dimension 0
- xvalid: int32 [128, 256], P('dp'), parts along dimension 0
- rowmask: int32 [128], P('dp'), parts along dimension 0
- self_attn_norm: bfloat16 [4096], replicated
- self_wq: bfloat16 [4096, 4096], P(None, 'tp')
- self_wk: bfloat16 [4096, 1024], P(None, 'tp')
- self_wv: bfloat16 [4096, 1024], P(None, 'tp')
- self_wo: bfloat16 [4096, 4096], P('tp')
- self_mlp_norm: bfloat16 [4096], replicated
- self_wgate: bfloat16 [4096, 14336], P(None, 'tp')
- self_wup: bfloat16 [4096, 14336], P(None, 'tp')
- self_wdown: bfloat16 [14336, 4096], P('tp')
- cross_attn_norm: bfloat16 [4096], replicated
- cross_wq: bfloat16 [4096, 4096], P(None, 'tp')
- cross_qnorm: bfloat16 [128], replicated
- cross_wo: bfloat16 [4096, 4096], P('tp')
- cross_gates: float32 [2], replicated
- cross_mlp_norm: bfloat16 [4096], replicated
- cross_wgate: bfloat16 [4096, 14336], P(None, 'tp')
- cross_wup: bfloat16 [4096, 14336], P(None, 'tp')
- cross_wdown: bfloat16 [14336, 4096], P('tp')
Outputs:
- output 1: bfloat16 [128, 4096], P('dp'), parts along dimension 0
- output 2: bfloat16 [128, 256, 8, 128], P('dp', 'sp', 'tp'), parts along dimension 0
- output 3: bfloat16 [128, 256, 8, 128], P('dp', 'sp', 'tp'), parts along dimension 0
There are 2 independent parts. The reference program is written for one: setup_inputs(seed, part) draws one part's arguments, and reference() takes and returns one part's arrays. A program takes and returns all parts, laid end to end along the dimension named above; an argument that names none is the same for every part.
All inputs are finite; a program needn't handle non-finite values.
Results may differ from the reference program's by a relative error of at most 0.0150412.
Values sent between devices are 32-bit elements.
A program may use at most 1 GiB of HBM per device.

```python
import math
import jax
import jax.numpy as jnp
from jax import lax

BATCH = 64
SEQ_LEN = 256
VIS_TOKENS = 256
HIDDEN = 4096
HEADS = 32
KV_HEADS = 8
HEAD_DIM = 128
MLP_DIM = 14336

GROUP_SIZE = HEADS // KV_HEADS
Q_WIDTH = HEADS * HEAD_DIM
KV_WIDTH = KV_HEADS * HEAD_DIM
NORM_EPS = 1e-5
ROPE_THETA = 500000.0
ROPE_FACTOR = 8.0
LOW_FREQ = 1.0
HIGH_FREQ = 4.0
ORIG_CTX = 8192.0
NEG_BIG = -1e30
KEY_SCALE = 1.6


def rope_freqs():
    inv_freq = 1.0 / (ROPE_THETA ** (jnp.arange(0, HEAD_DIM, 2).astype(jnp.float32) / HEAD_DIM))
    wavelen = 2.0 * math.pi / inv_freq
    smooth = (ORIG_CTX / wavelen - LOW_FREQ) / (HIGH_FREQ - LOW_FREQ)
    mid_freq = (1.0 - smooth) * inv_freq / ROPE_FACTOR + smooth * inv_freq
    scaled = jnp.where(wavelen > ORIG_CTX / LOW_FREQ, inv_freq / ROPE_FACTOR, mid_freq)
    return jnp.where(wavelen < ORIG_CTX / HIGH_FREQ, inv_freq, scaled)


def apply_rope(vectors, positions):
    half_dim = HEAD_DIM // 2
    angles = positions.astype(jnp.float32)[:, None] * rope_freqs()[None, :]
    cos_t = jnp.cos(angles)[:, None, :]
    sin_t = jnp.sin(angles)[:, None, :]
    first_half = vectors[..., :half_dim]
    second_half = vectors[..., half_dim:]
    return jnp.concatenate([first_half * cos_t - second_half * sin_t, second_half * cos_t + first_half * sin_t], axis=-1)


def rms_norm(values, gain_vec):
    vals32 = values.astype(jnp.float32)
    inv_rms = lax.rsqrt(jnp.mean(vals32 * vals32, axis=-1, keepdims=True) + NORM_EPS)
    return (vals32 * inv_rms * gain_vec.astype(jnp.float32)).astype(jnp.bfloat16)


def gated_mlp(normed, w_gate, w_up, w_down):
    gate_val = jnp.dot(normed, w_gate, preferred_element_type=jnp.float32).astype(jnp.bfloat16)
    up_val = jnp.dot(normed, w_up, preferred_element_type=jnp.float32).astype(jnp.bfloat16)
    hidden_act = (jax.nn.silu(gate_val.astype(jnp.float32)) * up_val.astype(jnp.float32)).astype(jnp.bfloat16)
    return jnp.dot(hidden_act, w_down, preferred_element_type=jnp.float32)


def attend_row(queries, key_rows, val_rows, valid_mask):
    scores = jnp.einsum('kgd,tkd->kgt', queries.astype(jnp.float32), key_rows.astype(jnp.float32)) * (HEAD_DIM ** -0.5)
    scores = jnp.where(valid_mask[None, None, :], scores, NEG_BIG)
    weights = jax.nn.softmax(scores, axis=-1)
    return jnp.einsum('kgt,tkd->kgd', weights, val_rows.astype(jnp.float32))


def attend_item(item):
    return attend_row(item[0], item[1], item[2], item[3])


def dense_weight(rand_key, rows, cols):
    return (jax.random.normal(rand_key, (rows, cols), jnp.float32) * (rows ** -0.5)).astype(jnp.bfloat16)


def norm_gain(rand_key, width, center):
    return (center + 0.35 * jax.random.normal(rand_key, (width,), jnp.float32)).astype(jnp.bfloat16)


def drifting_values(rand_key, length):
    noise_key, walk_key, dir_key = jax.random.split(rand_key, 3)
    noise_part = 0.6 * jax.random.normal(noise_key, (BATCH, length, KV_HEADS, HEAD_DIM), jnp.float32)
    walk_path = jnp.cumsum(jax.random.normal(walk_key, (BATCH, KV_HEADS, length), jnp.float32), axis=-1) * (length ** -0.5)
    direction = jax.random.normal(dir_key, (BATCH, KV_HEADS, HEAD_DIM), jnp.float32)
    return (noise_part + jnp.transpose(walk_path, (0, 2, 1))[:, :, :, None] * direction[:, None, :, :]).astype(jnp.bfloat16)


def setup_inputs(seed: int = 0, part: int = 0) -> dict:
    data_keys = jax.random.split(jax.random.fold_in(jax.random.key(seed), part), 12)
    weight_keys = jax.random.split(jax.random.key(seed + 1), 20)
    row_ids = jnp.arange(BATCH)
    new_pos = jax.random.randint(data_keys[0], (BATCH,), SEQ_LEN // 4, SEQ_LEN)
    new_pos = jnp.where(row_ids == 0, SEQ_LEN - 1, new_pos).astype(jnp.int32)
    rowmask = (jax.random.randint(data_keys[1], (BATCH,), 0, 4) > 0).astype(jnp.int32)
    rowmask = jnp.where(row_ids == 0, 1, jnp.where(row_ids == 1, 0, rowmask)).astype(jnp.int32)
    valid_len = jax.random.randint(data_keys[2], (BATCH,), VIS_TOKENS // 4, VIS_TOKENS + 1)
    valid_len = jnp.where(row_ids == 0, VIS_TOKENS, valid_len)
    xvalid = (jnp.arange(VIS_TOKENS)[None, :] < valid_len[:, None]).astype(jnp.int32)
    hidden = jax.random.normal(data_keys[3], (BATCH, HIDDEN), jnp.float32).astype(jnp.bfloat16)
    k_self = (KEY_SCALE * jax.random.normal(data_keys[4], (BATCH, SEQ_LEN, KV_HEADS, HEAD_DIM), jnp.float32)).astype(jnp.bfloat16)
    v_self = drifting_values(data_keys[5], SEQ_LEN)
    k_cross = (KEY_SCALE * jax.random.normal(data_keys[6], (BATCH, VIS_TOKENS, KV_HEADS, HEAD_DIM), jnp.float32)).astype(jnp.bfloat16)
    v_cross = drifting_values(data_keys[7], VIS_TOKENS)
    return dict(
        hidden=hidden,
        new_pos=new_pos,
        k_self=k_self,
        v_self=v_self,
        k_cross=k_cross,
        v_cross=v_cross,
        xvalid=xvalid,
        rowmask=rowmask,
        self_attn_norm=norm_gain(weight_keys[0], HIDDEN, 1.0),
        self_wq=dense_weight(weight_keys[1], HIDDEN, Q_WIDTH),
        self_wk=dense_weight(weight_keys[2], HIDDEN, KV_WIDTH),
        self_wv=dense_weight(weight_keys[3], HIDDEN, KV_WIDTH),
        self_wo=dense_weight(weight_keys[4], Q_WIDTH, HIDDEN),
        self_mlp_norm=norm_gain(weight_keys[5], HIDDEN, 1.0),
        self_wgate=dense_weight(weight_keys[6], HIDDEN, MLP_DIM),
        self_wup=dense_weight(weight_keys[7], HIDDEN, MLP_DIM),
        self_wdown=dense_weight(weight_keys[8], MLP_DIM, HIDDEN),
        cross_attn_norm=norm_gain(weight_keys[9], HIDDEN, 1.0),
        cross_wq=dense_weight(weight_keys[10], HIDDEN, Q_WIDTH),
        cross_qnorm=norm_gain(weight_keys[11], HEAD_DIM, 1.5),
        cross_wo=dense_weight(weight_keys[12], Q_WIDTH, HIDDEN),
        cross_gates=jax.random.uniform(weight_keys[13], (2,), jnp.float32, 0.5, 1.5),
        cross_mlp_norm=norm_gain(weight_keys[14], HIDDEN, 1.0),
        cross_wgate=dense_weight(weight_keys[15], HIDDEN, MLP_DIM),
        cross_wup=dense_weight(weight_keys[16], HIDDEN, MLP_DIM),
        cross_wdown=dense_weight(weight_keys[17], MLP_DIM, HIDDEN),
    )


def reference(hidden, new_pos, k_self, v_self, k_cross, v_cross, xvalid, rowmask,
              self_attn_norm, self_wq, self_wk, self_wv, self_wo, self_mlp_norm,
              self_wgate, self_wup, self_wdown, cross_attn_norm, cross_wq, cross_qnorm,
              cross_wo, cross_gates, cross_mlp_norm, cross_wgate, cross_wup, cross_wdown):
    normed = rms_norm(hidden, self_attn_norm)
    queries = jnp.dot(normed, self_wq, preferred_element_type=jnp.float32).astype(jnp.bfloat16)
    key_new = jnp.dot(normed, self_wk, preferred_element_type=jnp.float32).astype(jnp.bfloat16)
    val_new = jnp.dot(normed, self_wv, preferred_element_type=jnp.float32).astype(jnp.bfloat16)
    queries = apply_rope(queries.reshape(BATCH, HEADS, HEAD_DIM).astype(jnp.float32), new_pos).astype(jnp.bfloat16)
    key_new = apply_rope(key_new.reshape(BATCH, KV_HEADS, HEAD_DIM).astype(jnp.float32), new_pos).astype(jnp.bfloat16)
    val_new = val_new.reshape(BATCH, KV_HEADS, HEAD_DIM)
    slot_ids = jnp.arange(SEQ_LEN)
    hit_mask = (slot_ids[None, :] == new_pos[:, None])[:, :, None, None]
    k_new_cache = jnp.where(hit_mask, key_new[:, None], k_self)
    v_new_cache = jnp.where(hit_mask, val_new[:, None], v_self)
    seen_mask = slot_ids[None, :] <= new_pos[:, None]
    self_out = lax.map(attend_item, (queries.reshape(BATCH, KV_HEADS, GROUP_SIZE, HEAD_DIM), k_new_cache, v_new_cache, seen_mask))
    self_flat = self_out.astype(jnp.bfloat16).reshape(BATCH, Q_WIDTH)
    after_attn = (hidden.astype(jnp.float32) + jnp.dot(self_flat, self_wo, preferred_element_type=jnp.float32)).astype(jnp.bfloat16)
    mlp_out = gated_mlp(rms_norm(after_attn, self_mlp_norm), self_wgate, self_wup, self_wdown)
    after_mlp = (after_attn.astype(jnp.float32) + mlp_out).astype(jnp.bfloat16)
    normed = rms_norm(after_mlp, cross_attn_norm)
    cross_q = jnp.dot(normed, cross_wq, preferred_element_type=jnp.float32).astype(jnp.bfloat16)
    cross_q = rms_norm(cross_q.reshape(BATCH, HEADS, HEAD_DIM), cross_qnorm)
    cross_out = lax.map(attend_item, (cross_q.reshape(BATCH, KV_HEADS, GROUP_SIZE, HEAD_DIM), k_cross, v_cross, xvalid > 0))
    cross_flat = cross_out.astype(jnp.bfloat16).reshape(BATCH, Q_WIDTH)
    gate_vals = jnp.tanh(cross_gates.astype(jnp.float32))
    row_scale = rowmask.astype(jnp.float32)[:, None]
    cross_proj = jnp.dot(cross_flat, cross_wo, preferred_element_type=jnp.float32)
    after_cross = (after_mlp.astype(jnp.float32) + gate_vals[0] * row_scale * cross_proj).astype(jnp.bfloat16)
    xmlp_out = gated_mlp(rms_norm(after_cross, cross_mlp_norm), cross_wgate, cross_wup, cross_wdown)
    after_xmlp = (after_cross.astype(jnp.float32) + gate_vals[1] * row_scale * xmlp_out).astype(jnp.bfloat16)
    return (after_xmlp, k_new_cache, v_new_cache)
```

```python
import math
import numpy as np
import jax
import jax.numpy as jnp
from jax import lax
from jax.experimental import pallas as pl
from jax.experimental.pallas import tpu as pltpu
from jax.sharding import PartitionSpec as P

NORM_EPS = 1e-5
ROPE_THETA = 500000.0
ROPE_FACTOR = 8.0
LOW_FREQ = 1.0
HIGH_FREQ = 4.0
ORIG_CTX = 8192.0
NEG_BIG = -1e30
F32 = jnp.float32
BF16 = jnp.bfloat16
MESH_ID = pl.DeviceIdType.MESH

CW = 256
HD = 128
NH = 8
NQ = 4
ROWS = 64
NSP = 4
RB = 16
TBLK = 64
WIDTH = 4096
UNROLL = 8
VMEM_ALL = 67043328
NCH = 16
FF = 3584
QW = 1024
BLK3 = (RB, NH, HD)
NPAIR = 11
SEG_WO = (0, 2)
SEG_GU = (2, 14)
SEG_DN = (16, 8)
SEG_CQ = (24, 2)
SEG_CWO = (26, 2)
SEG_CGU = (28, 14)
SEG_CDN = (42, 8)


def rope_freqs(head_dim):
    f32 = np.float32
    inv_freq = (1.0 / (f32(ROPE_THETA) ** (np.arange(0, head_dim, 2).astype(f32) / f32(head_dim)))).astype(f32)
    wavelen = 2.0 * math.pi / inv_freq
    smooth = (ORIG_CTX / wavelen - LOW_FREQ) / (HIGH_FREQ - LOW_FREQ)
    mid_freq = (1.0 - smooth) * inv_freq / ROPE_FACTOR + smooth * inv_freq
    scaled = np.where(wavelen > ORIG_CTX / LOW_FREQ, inv_freq / ROPE_FACTOR, mid_freq)
    return np.where(wavelen < ORIG_CTX / HIGH_FREQ, inv_freq, scaled).astype(f32)


def blk(i, n):
    return pl.ds(pl.multiple_of(i * n, n), n)


def half_of(n, core):
    return pl.ds(n * 4 + 2 * core, 2)


def round_bf16(x):
    return x.astype(BF16).astype(F32)


def attend(queries, keys, values, limits, scale):
    scores = [lax.dot_general(q, k, (((1,), (1,)), ((), ())), preferred_element_type=F32)
              for q, k in zip(queries, keys)]
    lane = lax.broadcasted_iota(jnp.int32, scores[0].shape, 1)
    head = lax.broadcasted_iota(jnp.int32, scores[0].shape, 0)
    own = (lane & 1) == (head >> 2)
    slot = lane >> 1
    oks = [own & (slot < limit) for limit in limits]
    scores = [jnp.where(ok, sc * scale, NEG_BIG) for ok, sc in zip(oks, scores)]
    maxes = [jnp.max(sc, axis=1, keepdims=True) for sc in scores]
    probs = [jnp.where(ok, jnp.exp(sc - m), 0.0) for ok, sc, m in zip(oks, scores, maxes)]
    sums = [jnp.sum(p, axis=1, keepdims=True) for p in probs]
    outs = [jnp.dot(p.astype(BF16), v, preferred_element_type=F32) for p, v in zip(probs, values)]
    return maxes, sums, outs


def front_kernel(pos_ref, hid_hbm, g_ref, freq_ref, wq, wk, wv, k_hbm, v_hbm,
                 k_out, v_out, o_ref, st_ref,
                 hid, x, wbuf, kbuf, vbuf, qkv, gsc, tab, cosb, sinb,
                 wsem, hsem, ksem, vsem, kosem, vosem):
    base = lax.axis_index('sp') * TBLK
    hc = pltpu.make_async_copy(hid_hbm, hid, hsem)
    hc.start()
    for i in range(NQ):
        pltpu.make_async_copy(wq.at[:, pl.ds(i * CW, CW)], wbuf.at[i], wsem.at[i]).start(priority=1)
    pltpu.make_async_copy(wk, wbuf.at[NQ], wsem.at[NQ]).start(priority=1)
    pltpu.make_async_copy(wv, wbuf.at[NQ + 1], wsem.at[NQ + 1]).start(priority=1)

    def cache_copies(j, out):
        rows = pl.ds(j * RB, RB)
        if out:
            return (pltpu.make_async_copy(kbuf.at[rows], k_out.at[rows], kosem.at[j]),
                    pltpu.make_async_copy(vbuf.at[rows], v_out.at[rows], vosem.at[j]))
        return (pltpu.make_async_copy(k_hbm.at[rows], kbuf.at[rows], ksem.at[j]),
                pltpu.make_async_copy(v_hbm.at[rows], vbuf.at[rows], vsem.at[j]))

    for j in range(NSP):
        for cp in cache_copies(j, False):
            cp.start(priority=1)
    with jax.named_scope('tables'):
        gsc[...] = g_ref[...].astype(F32)

        def fill(r, carry):
            tab[pl.ds(r, 1), :] = jnp.full((1, HD), pos_ref[r], jnp.int32).astype(F32)
            return carry

        lax.fori_loop(0, ROWS, fill, 0, unroll=8)
        angle = tab[...] * freq_ref[...]
        lanes = lax.broadcasted_iota(jnp.int32, (ROWS, HD), 1)
        sin_v = jnp.sin(angle)
        cosb[...] = jnp.cos(angle)
        sinb[...] = jnp.where(lanes < HD // 2, -sin_v, sin_v)

    with jax.named_scope('norm'):
        hc.wait()

        def norm_rows(r, carry):
            rows = blk(r, RB)
            acc = jnp.zeros((RB, HD), F32)
            for j in range(WIDTH // HD):
                v = hid[rows, j * HD:(j + 1) * HD].astype(F32)
                acc = acc + v * v
            inv = lax.rsqrt(jnp.sum(acc, axis=-1, keepdims=True) * (1.0 / WIDTH) + NORM_EPS)
            for j in range(WIDTH // HD):
                cs = slice(j * HD, (j + 1) * HD)
                x[rows, cs] = (hid[rows, cs].astype(F32) * inv * gsc[j:j + 1, :]).astype(BF16)
            return carry

        lax.fori_loop(0, NSP, norm_rows, 0)

    with jax.named_scope('qkv'):
        def project(p, carry):
            for v in range(2):
                pltpu.make_async_copy(wk, wbuf.at[2 * p + v], wsem.at[2 * p + v]).wait()
            ys = [jnp.dot(x[...], wbuf[2 * p + v], preferred_element_type=F32) for v in range(2)]
            for v in range(2):
                yv = round_bf16(ys[v])
                for u in range(2):
                    part = yv[:, u * HD:(u + 1) * HD]
                    turned = round_bf16(part * cosb[...] + pltpu.roll(part, HD // 2, 1) * sinb[...])
                    if v == 1:
                        turned = jnp.where(p == NQ // 2, part, turned)
                    qkv[pl.ds(4 * p + 2 * v + u, ROWS, stride=RB), :] = turned
            return carry

        lax.fori_loop(0, NQ // 2 + 1, project, 0)

    scale = HD ** -0.5
    row_t = lax.broadcasted_iota(jnp.int32, (HD, HD), 0)
    lane8 = lax.broadcasted_iota(jnp.int32, (NH, HD), 1)
    head8 = lax.broadcasted_iota(jnp.int32, (NH, HD), 0)

    def put(buf, pair, b, lp):
        both = jnp.where((row_t & 1) == 0, pair[0:1, :], pair[1:2, :])
        upd = jnp.where((row_t >> 1) == lp, both, buf[b].astype(F32)).astype(BF16)
        buf[b] = upd
        return upd

    def some_rows(rows):
        lps = [pos_ref[b] - base for b in rows]
        fresh = [qkv[pl.ds(pl.multiple_of(b * RB + NH, NH), NH), :] for b in rows]
        queries = [qkv[pl.ds(pl.multiple_of(b * RB, RB), NH), :].astype(BF16) for b in rows]
        keys = [put(kbuf, f[0:2], b, lp) for f, b, lp in zip(fresh, rows, lps)]
        values = [put(vbuf, f[2:4], b, lp) for f, b, lp in zip(fresh, rows, lps)]
        maxes, sums, outs = attend(queries, keys, values, [lp + 1 for lp in lps], scale)
        for b, m, l, o in zip(rows, maxes, sums, outs):
            o_ref[blk(b, NH), :] = o
            st = jnp.where(lane8 == head8, m, 0.0) + jnp.where(lane8 == head8 + NH, l, 0.0)
            st_ref[pl.ds(b, 1), :] = jnp.sum(st, axis=0, keepdims=True)

    with jax.named_scope('attend'):
        def block(j, carry):
            for cp in cache_copies(j, False):
                cp.wait()

            def some(i, carry2):
                some_rows([j * RB + i * UNROLL + u for u in range(UNROLL)])
                return carry2

            lax.fori_loop(0, RB // UNROLL, some, 0)
            for cp in cache_copies(j, True):
                cp.start()
            return carry

        lax.fori_loop(0, NSP, block, 0)
    with jax.named_scope('flush'):
        for j in range(NSP):
            for cp in cache_copies(j, True):
                cp.wait()


def back_kernel(mask_ref, gates_ref, o_part, stats, hid_hbm, xv_hbm, g2_ref, g3_ref, g4_ref, qn_ref,
                wo, wg, wu, wd, cq, cwo, cg, cu, cd, kc_hbm, vc_hbm,
                out_ref,
                ring, kc, vc, hidb, xvb, cnt, gab, gmb, gsc, hres, xb, ab, ofl, osc, qsc, ro, rst, pb, r1, sb, r2, tb, full,
                rsem, csem, hsem, xsem, osem, stsem, a1s, a1r, a2s, a2r, a3s, a3r, zss, zrs, yss, yrs, dss, drs):
    s = lax.axis_index('sp')
    t = lax.axis_index('tp')
    c = lax.rem(t, 2)
    y = lax.div(t, 2)
    core_peer = {'tp': t + 1 - 2 * c}
    y_peer = {'tp': lax.rem(t + 2, 4)}
    sp_peers = [lax.rem(s + k, 4) for k in (1, 2, 3)]
    sp_from = [lax.rem(s + 4 - k, 4) for k in (1, 2, 3)]

    def cols(w, j):
        return w.at[:, blk(j, CW)]

    def tall(w, slot, sub, j):
        return [(cols(w, j), ring.at[slot, sub, pl.ds(0, w.shape[0])])]

    def square(w, slot, sub, j):
        rows = w.shape[0]
        return [(cols(w, 4 * j + k), ring.at[slot, sub, pl.ds(k * rows, rows)]) for k in range(4)]

    segments = (
        (SEG_WO, lambda sl, p: square(wo, sl, 0, 2 * p), lambda sl, p: square(wo, sl, 1, 2 * p + 1)),
        (SEG_GU, lambda sl, p: tall(wg, sl, 0, p), lambda sl, p: tall(wu, sl, 1, p)),
        (SEG_DN, lambda sl, p: tall(wd, sl, 0, 2 * p), lambda sl, p: tall(wd, sl, 1, 2 * p + 1)),
        (SEG_CQ, lambda sl, p: tall(cq, sl, 0, 2 * p), lambda sl, p: tall(cq, sl, 1, 2 * p + 1)),
        (SEG_CWO, lambda sl, p: square(cwo, sl, 0, 2 * p), lambda sl, p: square(cwo, sl, 1, 2 * p + 1)),
        (SEG_CGU, lambda sl, p: tall(cg, sl, 0, p), lambda sl, p: tall(cu, sl, 1, p)),
        (SEG_CDN, lambda sl, p: tall(cd, sl, 0, 2 * p), lambda sl, p: tall(cd, sl, 1, 2 * p + 1)),
    )

    def issue(pair, low, high):
        slot = lax.rem(pair, NPAIR)
        for (first, count), even, odd in segments:
            if first >= high or first + count <= low:
                continue

            def go(first=first, even=even, odd=odd):
                for sub, make in ((0, even), (1, odd)):
                    for src, dst in make(slot, pair - first):
                        pltpu.make_async_copy(src, dst, rsem.at[slot, sub]).start(priority=1)

            if first <= low and high <= first + count:
                go()
            else:
                pl.when((pair >= first) & (pair < first + count))(go)

    def arrive(slot, sub, rows):
        dst = ring.at[slot, sub, pl.ds(0, rows)]
        pltpu.make_async_copy(dst, dst, rsem.at[slot, sub]).wait()

    def send1(ar, n):
        return pltpu.make_async_remote_copy(
            pb.at[ar, half_of(n, 1 - c)], r1.at[ar, n], a1s.at[ar, n], a1r.at[ar, n],
            device_id=core_peer, device_id_type=MESH_ID)

    def send2(ar, n):
        return pltpu.make_async_remote_copy(
            sb.at[ar, n], r2.at[ar, n], a2s.at[ar, n], a2r.at[ar, n],
            device_id=y_peer, device_id_type=MESH_ID)

    def send3(ar, n):
        mine = tb.at[ar, half_of(n, c)]
        return pltpu.make_async_remote_copy(
            mine, mine, a3s.at[ar, n], a3r.at[ar, n], device_id=core_peer, device_id_type=MESH_ID)

    def stage2(ar, n):
        send1(ar, n).wait_recv()
        sb[ar, n] = pb[ar, half_of(n, c)] + r1[ar, n]
        send2(ar, n).start()

    def stage3(ar, n):
        send2(ar, n).wait_recv()
        tb[ar, half_of(n, c)] = sb[ar, n] + r2[ar, n]
        send3(ar, n).start()

    def to_sp(n, k):
        mine = full.at[s, half_of(n, c)]
        i = lax.div(n, 2)
        return pltpu.make_async_remote_copy(
            mine, mine, zss.at[i, k], zrs.at[i, k], device_id={'sp': sp_peers[k]}, device_id_type=MESH_ID)

    def from_sp(i, k):
        got = full.at[sp_from[k], half_of(2 * i + y, c)]
        return got, pltpu.make_async_remote_copy(
            got, got, zss.at[i, k], zrs.at[i, k], device_id={'sp': sp_peers[k]}, device_id_type=MESH_ID)

    def to_y(i, k):
        got = full.at[sp_from[k], half_of(2 * i + y, c)]
        return pltpu.make_async_remote_copy(
            got, got, yss.at[i, k], yrs.at[i, k], device_id=y_peer, device_id_type=MESH_ID)

    def to_core(piece, idx):
        return pltpu.make_async_remote_copy(
            piece, piece, dss.at[idx], drs.at[idx], device_id=core_peer, device_id_type=MESH_ID)

    def own_piece(n):
        return full.at[s, half_of(n, c)]

    def final3(ar, n):
        send2(ar, n).wait_recv()
        gm = gmb[...]
        for u in range(2):
            piece = n * 4 + 2 * c + u
            total = sb[ar, n, u] + r2[ar, n, u]
            for w in range(2):
                cs = slice(w * HD, (w + 1) * HD)
                full[s, piece, :, cs] = round_bf16(hres[piece][:, cs] + gm * total[:, cs])
        to_core(own_piece(n), n).start()

        @pl.when(lax.rem(n, 2) == y)
        def _():
            for k in range(3):
                to_sp(n, k).start()

    def advance(ar, n, last=False):
        send1(ar, n).start()

        @pl.when(n >= 1)
        def _():
            stage2(ar, n - 1)

        @pl.when(n >= 2)
        def _():
            (final3 if last else stage3)(ar, n - 2)

    def drain(ar, last=False):
        third = final3 if last else stage3
        third(ar, 2)
        third(ar, 3)
        for n in range(4):
            if not last:
                send3(ar, n).wait_recv()
            send1(ar, n).wait_send()
            send2(ar, n).wait_send()
            if not last:
                send3(ar, n).wait_send()

    def norm(g_ref, update):
        gsc[...] = g_ref[...].astype(F32)

        def add(q, acc):
            v = update(q)
            hres[q] = v
            return acc + v * v

        acc = lax.fori_loop(0, NCH, add, jnp.zeros((RB, CW), F32), unroll=4)
        inv = lax.rsqrt(jnp.sum(acc, axis=-1, keepdims=True) * (1.0 / WIDTH) + NORM_EPS)

        def put(q, carry):
            for u in range(2):
                cs = slice(u * HD, (u + 1) * HD)
                v = hres[q][:, cs] * inv * gsc[pl.ds(2 * q + u, 1), :]
                xb[:, pl.ds(pl.multiple_of(q * CW + u * HD, HD), HD)] = v.astype(BF16)
            return carry

        lax.fori_loop(0, NCH, put, 0, unroll=4)

    def project_out(ar, seg):
        first = seg[0]

        def pair(p, carry):
            slot = lax.rem(first + p, NPAIR)
            for sub in range(2):
                n = 2 * p + sub
                arrive(slot, sub, WIDTH)
                ps = [jnp.dot(ofl[...], ring[slot, sub, k * QW:(k + 1) * QW, :], preferred_element_type=F32)
                      for k in range(4)]
                for k in range(4):
                    pb[ar, n * 4 + k] = ps[k]
                send1(ar, n).start()
            issue(first + p + NPAIR, first + NPAIR, first + NPAIR + 2)
            return carry

        lax.fori_loop(0, 2, pair, 0)
        for n in range(3):
            stage2(ar, n)
        stage2(ar, 3)
        stage3(ar, 0)
        stage3(ar, 1)
        drain(ar)

    def gate_up(seg):
        first = seg[0]

        def pair(p, carry):
            slot = lax.rem(first + p, NPAIR)
            for sub in range(2):
                arrive(slot, sub, WIDTH)
            gate, up = [jnp.dot(xb[...], ring[slot, sub], preferred_element_type=F32) for sub in range(2)]
            gate, up = round_bf16(gate), round_bf16(up)
            act = (gate * jax.nn.sigmoid(gate) * up).astype(BF16)
            ab[:, blk(p, CW)] = act
            issue(first + p + NPAIR, first + NPAIR, first + NPAIR + seg[1])
            return carry

        lax.fori_loop(0, seg[1], pair, 0)

    def down(ar, seg, last=False):
        first = seg[0]

        def group(n, carry):
            def pair(p, carry2):
                idx = first + 2 * n + p
                slot = lax.rem(idx, NPAIR)
                for sub in range(2):
                    arrive(slot, sub, FF)
                both = [jnp.dot(ab[...], ring[slot, sub, :FF, :], preferred_element_type=F32) for sub in range(2)]
                for sub in range(2):
                    pb[ar, n * 4 + 2 * p + sub] = both[sub]
                if not last:
                    issue(idx + NPAIR, first + NPAIR, first + NPAIR + seg[1])
                return carry2

            lax.fori_loop(0, 2, pair, 0)
            advance(ar, n, last)
            return carry

        lax.fori_loop(0, 4, group, 0)
        stage2(ar, 3)
        drain(ar, last)

    def heads_to_rows():
        for h in range(8):
            ofl[:, h * 128:(h + 1) * 128] = osc[pl.ds(h, 16, stride=8), :].astype(BF16)

    hcopy = pltpu.make_async_copy(hid_hbm.at[blk(s, RB)], hidb, hsem)
    hcopy.start()
    xcopy = pltpu.make_async_copy(xv_hbm.at[blk(s, RB)], xvb, xsem)
    xcopy.start()
    for p in range(5):
        issue(p, p, p + 1)
    barrier = pltpu.get_barrier_semaphore()
    for peer in [core_peer, y_peer] + [{'sp': v} for v in sp_peers]:
        pl.semaphore_signal(barrier, inc=1, device_id=peer, device_id_type=MESH_ID)
    pl.semaphore_wait(barrier, 5)

    def part_copy(k):
        rows = blk(sp_peers[k], HD)
        srow = blk(sp_peers[k], RB)
        to = {'sp': sp_peers[k]}
        return (pltpu.make_async_remote_copy(o_part.at[rows], ro.at[k], osem.at[0, k], osem.at[1, k],
                                             device_id=to, device_id_type=MESH_ID),
                pltpu.make_async_remote_copy(stats.at[srow], rst.at[k], stsem.at[0, k], stsem.at[1, k],
                                             device_id=to, device_id_type=MESH_ID))

    for k in (2, 1, 0):
        for cp in part_copy(k):
            cp.start()
    for p in range(5, NPAIR):
        issue(p, p, p + 1)
    for r in range(RB):
        on = jnp.full((1, HD), mask_ref[s * RB + r], jnp.int32).astype(F32)
        gab[r:r + 1, :] = on
    on = gab[...]
    gab[...] = jnp.tanh(jnp.full((RB, HD), gates_ref[0], F32)) * on
    gmb[...] = jnp.tanh(jnp.full((RB, HD), gates_ref[1], F32)) * on
    xcopy.wait()
    cnt[...] = jnp.broadcast_to(jnp.sum((xvb[...] > 0).astype(jnp.int32), axis=1, keepdims=True), (RB, HD))
    with jax.named_scope('parts'):
        for k in range(3):
            for cp in part_copy(k):
                cp.wait()

    lane3 = lax.broadcasted_iota(jnp.int32, BLK3, 2)
    head3 = lax.broadcasted_iota(jnp.int32, BLK3, 1)

    def pick(st, off):
        return jnp.sum(jnp.where(lane3 == head3 + off, st[:, None, :], 0.0), axis=2, keepdims=True)

    parts = [(o_part[blk(s, HD), :], stats[blk(s, RB), :])]
    parts += [(ro[k], rst[k]) for k in range(3)]
    maxes = [pick(st, 0) for _, st in parts]
    top = jnp.maximum(jnp.maximum(maxes[0], maxes[1]), jnp.maximum(maxes[2], maxes[3]))
    total = jnp.zeros(BLK3, F32)
    denom = jnp.zeros((16, 8, 1), F32)
    for (o, st), m in zip(parts, maxes):
        f = jnp.exp(m - top)
        denom = denom + pick(st, 8) * f
        total = total + o.reshape(BLK3) * f
    osc[...] = (total / denom).reshape(HD, HD)
    heads_to_rows()
    hcopy.wait()

    with jax.named_scope('wo'):
        project_out(0, SEG_WO)
    with jax.named_scope('norm2'):
        norm(g2_ref, lambda q: round_bf16(
            hidb[:, blk(q, CW)].astype(F32) + tb[0, q]))
    with jax.named_scope('gu'):
        gate_up(SEG_GU)
    rows16 = blk(s, RB)
    kcopy = pltpu.make_async_copy(kc_hbm.at[rows16], kc, csem.at[0])
    vcopy = pltpu.make_async_copy(vc_hbm.at[rows16], vc, csem.at[1])
    kcopy.start(priority=1)
    vcopy.start(priority=1)
    with jax.named_scope('dn'):
        down(1, SEG_DN)
    with jax.named_scope('norm3'):
        norm(g3_ref, lambda q: round_bf16(hres[q] + tb[1, q]))

    qn = qn_ref[...].astype(F32)
    first_q = SEG_CQ[0]
    with jax.named_scope('cq'):
        def queries(p, carry):
            slot = lax.rem(first_q + p, NPAIR)
            for sub in range(2):
                arrive(slot, sub, WIDTH)
            both = [jnp.dot(xb[...], ring[slot, sub], preferred_element_type=F32) for sub in range(2)]
            for sub in range(2):
                part = round_bf16(both[sub])
                for u in range(2):
                    v = part[:, u * HD:(u + 1) * HD]
                    inv = lax.rsqrt(jnp.mean(v * v, axis=-1, keepdims=True) + NORM_EPS)
                    qsc[pl.ds(4 * p + 2 * sub + u, RB, stride=NH), :] = round_bf16(v * inv * qn)
            issue(first_q + p + NPAIR, first_q + NPAIR, first_q + NPAIR + 2)
            return carry

        lax.fori_loop(0, 2, queries, 0)

    with jax.named_scope('cross'):
        kcopy.wait()
        vcopy.wait()

        def cross_rows(i, carry):
            bs = [i * 4 + u for u in range(4)]
            rows = [blk(b, NH) for b in bs]
            _, sums, outs = attend([qsc[r, :].astype(BF16) for r in rows], [kc[b] for b in bs], [vc[b] for b in bs],
                                   [cnt[pl.ds(b, 1), 0:1] for b in bs], HD ** -0.5)
            for r, l, o in zip(rows, sums, outs):
                osc[r, :] = o / l
            return carry

        lax.fori_loop(0, 4, cross_rows, 0)
        heads_to_rows()
    with jax.named_scope('cwo'):
        project_out(2, SEG_CWO)
    with jax.named_scope('norm4'):
        ga = jnp.concatenate([gab[...], gab[...]], axis=1)
        norm(g4_ref, lambda q: round_bf16(hres[q] + ga * tb[2, q]))
    with jax.named_scope('cgu'):
        gate_up(SEG_CGU)
    with jax.named_scope('cdn'):
        down(3, SEG_CDN, last=True)

    with jax.named_scope('spread'):
        for i in range(2):
            for k in range(3):
                got, cp = from_sp(i, k)
                cp.wait_recv()
                to_y(i, k).start()
                to_core(got, 4 + 3 * i + k).start()
        for i in range(2):
            for k in range(3):
                to_y(i, k).wait_recv()
                other = full.at[sp_from[k], half_of(2 * i + 1 - y, c)]
                to_core(other, 10 + 3 * i + k).start()
        for idx in range(16):
            to_core(own_piece(0), idx).wait()
        for i in range(2):
            for k in range(3):
                to_sp(2 * i, k).wait_send()
                to_y(i, k).wait_send()
    with jax.named_scope('emit'):
        def emit(q, carry):
            for r in range(NSP):
                out_ref[r * RB:(r + 1) * RB, blk(q, CW)] = full[r, q].astype(BF16)
            return carry

        lax.fori_loop(0, NCH, emit, 0, unroll=2)


def solution(mesh):
    cache_spec = P('dp', 'sp', 'tp', None)
    cross_spec = P('dp', None, 'tp', None)
    row_spec = P('dp', None)
    vec_spec = P('dp')
    full_spec = P(None)
    col_spec = P(None, 'tp')
    split_rows = P('tp', None)
    in_specs = (row_spec, vec_spec, cache_spec, cache_spec, cross_spec, cross_spec, row_spec, vec_spec,
                full_spec, col_spec, col_spec, col_spec, split_rows, full_spec, col_spec, col_spec, split_rows,
                full_spec, col_spec, full_spec, split_rows, full_spec, full_spec, col_spec, col_spec, split_rows)
    out_specs = (row_spec, cache_spec, cache_spec)
    vmem = pl.BlockSpec(memory_space=pltpu.VMEM)
    smem = pl.BlockSpec(memory_space=pltpu.SMEM)
    hbm = pl.BlockSpec(memory_space=pl.ANY)
    dma = pltpu.SemaphoreType.DMA

    def local_step(hidden, new_pos, k_self, v_self, k_cross, v_cross, xvalid, rowmask,
                   self_attn_norm, self_wq, self_wk, self_wv, self_wo, self_mlp_norm,
                   self_wgate, self_wup, self_wdown, cross_attn_norm, cross_wq, cross_qnorm,
                   cross_wo, cross_gates, cross_mlp_norm, cross_wgate, cross_wup, cross_wdown):
        half = rope_freqs(HD)
        freq = np.concatenate([half, half]).reshape(1, HD).astype(np.float32)

        def fold(gain):
            return gain.reshape(WIDTH // HD, HD)

        k_new, v_new, o_part, stats = pl.pallas_call(
            front_kernel,
            out_shape=(*[jax.ShapeDtypeStruct((ROWS, HD, HD), BF16)] * 2,
                       jax.ShapeDtypeStruct((ROWS * NH, HD), F32), jax.ShapeDtypeStruct((ROWS, HD), F32)),
            in_specs=[smem, hbm, vmem, vmem, hbm, hbm, hbm, hbm, hbm],
            out_specs=(hbm, hbm, vmem, vmem),
            scratch_shapes=[
                *[pltpu.VMEM((ROWS, WIDTH), BF16)] * 2, pltpu.VMEM((NQ + 2, WIDTH, CW), BF16),
                *[pltpu.VMEM((ROWS, HD, HD), BF16)] * 2,
                pltpu.VMEM((ROWS * RB, HD), F32), pltpu.VMEM((WIDTH // HD, HD), F32),
                *[pltpu.VMEM((ROWS, HD), F32)] * 3,
                dma((NQ + 2,)), dma, *[dma((NSP,))] * 4],
            compiler_params=pltpu.CompilerParams(vmem_limit_bytes=VMEM_ALL),
            name='front',
        )(new_pos, hidden, fold(self_attn_norm), jnp.asarray(freq), self_wq, self_wk, self_wv,
          k_self.reshape(ROWS, HD, HD), v_self.reshape(ROWS, HD, HD))

        out = pl.pallas_call(
            back_kernel,
            out_shape=jax.ShapeDtypeStruct((ROWS, WIDTH), BF16),
            in_specs=[smem, smem, vmem, vmem, hbm, hbm] + [vmem] * 4 + [hbm] * 11,
            out_specs=vmem,
            scratch_shapes=[
                pltpu.VMEM((NPAIR, 2, WIDTH, CW), BF16),
                *[pltpu.VMEM((RB, 512, HD), BF16)] * 2,
                pltpu.VMEM((RB, WIDTH), BF16), pltpu.VMEM((RB, 256), jnp.int32), pltpu.VMEM((RB, HD), jnp.int32),
                pltpu.VMEM((RB, HD), F32), pltpu.VMEM((RB, HD), F32), pltpu.VMEM((WIDTH // HD, HD), F32),
                pltpu.VMEM((NCH, RB, CW), F32),
                pltpu.VMEM((RB, WIDTH), BF16), pltpu.VMEM((RB, FF), BF16), pltpu.VMEM((RB, QW), BF16),
                *[pltpu.VMEM((HD, HD), F32)] * 2, pltpu.VMEM((3, HD, HD), F32), pltpu.VMEM((3, RB, HD), F32),
                pltpu.VMEM((4, NCH, RB, CW), F32), *[pltpu.VMEM((4, 4, 2, RB, CW), F32)] * 3,
                *[pltpu.VMEM((4, NCH, RB, CW), F32)] * 2,
                dma((NPAIR, 2)), dma((2,)), dma, dma, *[dma((2, 3))] * 2,
                *[dma((4, 4))] * 6,
                *[dma((2, 3))] * 4, dma((NCH,)), dma((NCH,))],
            compiler_params=pltpu.CompilerParams(
                collective_id=0, has_side_effects=True, vmem_limit_bytes=VMEM_ALL),
            name='back',
        )(rowmask, cross_gates, o_part, stats, hidden, xvalid, fold(self_mlp_norm), fold(cross_attn_norm),
          fold(cross_mlp_norm), cross_qnorm.reshape(1, -1),
          self_wo, self_wgate, self_wup, self_wdown, cross_wq, cross_wo, cross_wgate, cross_wup, cross_wdown,
          *[cache.reshape(ROWS, -1, HD) for cache in (k_cross, v_cross)])
        return out, k_new.reshape(k_self.shape), v_new.reshape(v_self.shape)

    return jax.shard_map(local_step, mesh=mesh, in_specs=in_specs, out_specs=out_specs, check_vma=False)
```

```python
import math
import numpy as np
import jax
import jax.numpy as jnp
from jax import lax
from jax.experimental import pallas as pl
from jax.experimental.pallas import tpu as pltpu
from jax.sharding import PartitionSpec as P

NORM_EPS = 1e-5
ROPE_THETA = 500000.0
ROPE_FACTOR = 8.0
LOW_FREQ = 1.0
HIGH_FREQ = 4.0
ORIG_CTX = 8192.0
NEG_BIG = -1e30
F32 = jnp.float32
BF16 = jnp.bfloat16
MESH_ID = pl.DeviceIdType.MESH

CW = 256
HD = 128
NH = 8
NQ = 4
ROWS = 64
NSP = 4
RB = 16
TBLK = 64
WIDTH = 4096
UNROLL = 8
VMEM_ALL = 67043328
NCH = 16
FF = 3584
QW = 1024
LAST = 3
NG = 8
SP_ORDER = (2, 1, 0)
BLK3 = (RB, NH, HD)
NPAIR = 12
SEG_QKV = (0, 3)
SEG_WO = (3, 2)
SEG_GU = (5, 14)
SEG_DN = (19, 8)
SEG_CQ = (27, 2)
SEG_CWO = (29, 2)
SEG_CGU = (31, 14)
SEG_CDN = (45, 8)


def rope_freqs(head_dim):
    f32 = np.float32
    inv_freq = (1.0 / (f32(ROPE_THETA) ** (np.arange(0, head_dim, 2).astype(f32) / f32(head_dim)))).astype(f32)
    wavelen = 2.0 * math.pi / inv_freq
    smooth = (ORIG_CTX / wavelen - LOW_FREQ) / (HIGH_FREQ - LOW_FREQ)
    mid_freq = (1.0 - smooth) * inv_freq / ROPE_FACTOR + smooth * inv_freq
    scaled = np.where(wavelen > ORIG_CTX / LOW_FREQ, inv_freq / ROPE_FACTOR, mid_freq)
    return np.where(wavelen < ORIG_CTX / HIGH_FREQ, inv_freq, scaled).astype(f32)


def blk(i, n):
    return pl.ds(pl.multiple_of(i * n, n), n)


def half_of(n, core):
    return pl.ds(n * 4 + 2 * core, 2)


def round_bf16(x):
    return x.astype(BF16).astype(F32)


def attend(queries, keys, values, limits, scale):
    scores = [lax.dot_general(q, k, (((1,), (1,)), ((), ())), preferred_element_type=F32)
              for q, k in zip(queries, keys)]
    lane = lax.broadcasted_iota(jnp.int32, scores[0].shape, 1)
    head = lax.broadcasted_iota(jnp.int32, scores[0].shape, 0)
    own = (lane & 1) == (head >> 2)
    slot = lane >> 1
    oks = [own & (slot < limit) for limit in limits]
    scores = [jnp.where(ok, sc * scale, NEG_BIG) for ok, sc in zip(oks, scores)]
    maxes = [jnp.max(sc, axis=1, keepdims=True) for sc in scores]
    probs = [jnp.where(ok, jnp.exp(sc - m), 0.0) for ok, sc, m in zip(oks, scores, maxes)]
    sums = [jnp.sum(p, axis=1, keepdims=True) for p in probs]
    outs = [jnp.dot(p.astype(BF16), v, preferred_element_type=F32) for p, v in zip(probs, values)]
    return maxes, sums, outs


def with_new(rows, pair, lp):
    row_t = lax.broadcasted_iota(jnp.int32, (HD, HD), 0)
    both = jnp.where((row_t & 1) == 0, pair[0:1, :], pair[1:2, :])
    return jnp.where((row_t >> 1) == lp, both, rows.astype(F32)).astype(BF16)


def step_kernel(pos_ref, mask_ref, gates_ref, hid_hbm, xv_hbm, g1_ref, g2_ref, g3_ref, g4_ref, qn_ref, freq_ref,
                k_hbm, v_hbm, wq, wk, wv, wo, wg, wu, wd, cq, cwo, cg, cu, cd, kc_hbm, vc_hbm,
                full, fresh,
                ring, kbuf, vbuf, hid, x, tab, cosb, sinb, qself, o_part, stats,
                xvb, cnt, gab, gmb, gsc, hres, xb, ab, ofl, osc, qsc, ro, rst, pb, r1, sb, r2, tb, l1, lsum, l2,
                rsem, csem, hsem, xsem, ksem, vsem, osem, stsem, a1s, a1r, a2s, a2r, a3s, a3r,
                b1s, b1r, b2s, b2r, os_, or_, zss, zrs, yss, yrs, dss, drs):
    s = lax.axis_index('sp')
    t = lax.axis_index('tp')
    c = lax.rem(t, 2)
    y = lax.div(t, 2)
    core_peer = {'tp': t + 1 - 2 * c}
    y_peer = {'tp': lax.rem(t + 2, 4)}
    sp_peers = [lax.rem(s + k, 4) for k in (1, 2, 3)]
    sp_from = [lax.rem(s + 4 - k, 4) for k in (1, 2, 3)]

    def cols(w, j):
        return w.at[:, blk(j, CW)]

    def tall(w, slot, sub, j):
        return [(cols(w, j), ring.at[slot, sub, pl.ds(0, w.shape[0])])]

    def square(w, slot, sub, j):
        rows = w.shape[0]
        return [(cols(w, 4 * j + k), ring.at[slot, sub, pl.ds(k * rows, rows)]) for k in range(4)]

    segments = (
        (SEG_WO, lambda sl, p: square(wo, sl, 0, 2 * p), lambda sl, p: square(wo, sl, 1, 2 * p + 1)),
        (SEG_GU, lambda sl, p: tall(wg, sl, 0, p), lambda sl, p: tall(wu, sl, 1, p)),
        (SEG_DN, lambda sl, p: tall(wd, sl, 0, 2 * p), lambda sl, p: tall(wd, sl, 1, 2 * p + 1)),
        (SEG_CQ, lambda sl, p: tall(cq, sl, 0, 2 * p), lambda sl, p: tall(cq, sl, 1, 2 * p + 1)),
        (SEG_CWO, lambda sl, p: square(cwo, sl, 0, 2 * p), lambda sl, p: square(cwo, sl, 1, 2 * p + 1)),
        (SEG_CGU, lambda sl, p: tall(cg, sl, 0, p), lambda sl, p: tall(cu, sl, 1, p)),
        (SEG_CDN, lambda sl, p: tall(cd, sl, 0, 2 * p), lambda sl, p: tall(cd, sl, 1, 2 * p + 1)),
    )

    def issue(pair, low, high):
        slot = lax.rem(pair, NPAIR)
        for (first, count), even, odd in segments:
            if first >= high or first + count <= low:
                continue

            def go(first=first, even=even, odd=odd):
                for sub, make in ((0, even), (1, odd)):
                    for src, dst in make(slot, pair - first):
                        pltpu.make_async_copy(src, dst, rsem.at[slot, sub]).start(priority=1)

            if first <= low and high <= first + count:
                go()
            else:
                pl.when((pair >= first) & (pair < first + count))(go)

    def arrive(slot, sub, rows):
        dst = ring.at[slot, sub, pl.ds(0, rows)]
        pltpu.make_async_copy(dst, dst, rsem.at[slot, sub]).wait()

    def send1(ar, n):
        return pltpu.make_async_remote_copy(
            pb.at[ar, half_of(n, 1 - c)], r1.at[ar, n], a1s, a1r.at[n],
            device_id=core_peer, device_id_type=MESH_ID)

    def send2(ar, n):
        return pltpu.make_async_remote_copy(
            sb.at[ar, n], r2.at[ar, n], a2s, a2r.at[ar % 2, n],
            device_id=y_peer, device_id_type=MESH_ID)

    def send3(ar, n):
        mine = tb.at[ar, half_of(n, c)]
        return pltpu.make_async_remote_copy(
            mine, mine, a3s, a3r.at[n], device_id=core_peer, device_id_type=MESH_ID)

    def stage2(ar, n):
        send1(ar, n).wait_recv()
        sb[ar, n] = pb[ar, half_of(n, c)] + r1[ar, n]
        send2(ar, n).start()

    def stage3(ar, n):
        send2(ar, n).wait_recv()
        tb[ar, half_of(n, c)] = sb[ar, n] + r2[ar, n]
        send3(ar, n).start()

    def drain(ar):
        stage3(ar, 2)
        stage3(ar, 3)
        for n in range(4):
            send3(ar, n).wait_recv()
        sent(pb.at[ar, pl.ds(0, NH)], a1s)
        sent(pb.at[ar, pl.ds(0, NH)], a2s)
        sent(pb.at[ar, pl.ds(0, NH)], a3s)

    def sent(ref, sem):
        pltpu.make_async_copy(ref, ref, sem).wait()

    def norm(g_ref, update):
        gsc[...] = g_ref[...].astype(F32)

        def add(q, acc):
            v = update(q)
            hres[q] = v
            return acc + v * v

        acc = lax.fori_loop(0, NCH, add, jnp.zeros((RB, CW), F32), unroll=4)
        inv = lax.rsqrt(jnp.sum(acc, axis=-1, keepdims=True) * (1.0 / WIDTH) + NORM_EPS)

        def put(q, carry):
            for u in range(2):
                cs = slice(u * HD, (u + 1) * HD)
                v = hres[q][:, cs] * inv * gsc[pl.ds(2 * q + u, 1), :]
                xb[:, pl.ds(pl.multiple_of(q * CW + u * HD, HD), HD)] = v.astype(BF16)
            return carry

        lax.fori_loop(0, NCH, put, 0, unroll=4)

    def project_out(ar, seg):
        first = seg[0]

        def pair(p, carry):
            slot = lax.rem(first + p, NPAIR)
            for sub in range(2):
                n = 2 * p + sub
                arrive(slot, sub, WIDTH)
                ps = [jnp.dot(ofl[...], ring[slot, sub, k * QW:(k + 1) * QW, :], preferred_element_type=F32)
                      for k in range(4)]
                for k in range(4):
                    pb[ar, n * 4 + k] = ps[k]
                send1(ar, n).start()
            issue(first + p + NPAIR, first + NPAIR, first + NPAIR + 2)
            return carry

        lax.fori_loop(0, 2, pair, 0)
        for n in range(3):
            stage2(ar, n)
        stage2(ar, 3)
        stage3(ar, 0)
        stage3(ar, 1)
        drain(ar)

    def gate_up(seg):
        first = seg[0]

        def two(p, carry):
            pairs = [2 * p, 2 * p + 1]
            slots = [lax.rem(first + j, NPAIR) for j in pairs]
            for slot in slots:
                for sub in range(2):
                    arrive(slot, sub, WIDTH)
            prods = [[jnp.dot(xb[...], ring[slot, sub], preferred_element_type=F32) for sub in range(2)]
                     for slot in slots]
            for j, (gate, up) in zip(pairs, prods):
                gate, up = round_bf16(gate), round_bf16(up)
                ab[:, blk(j, CW)] = (gate * jax.nn.sigmoid(gate) * up).astype(BF16)
            for j in pairs:
                issue(first + j + NPAIR, first + NPAIR, first + NPAIR + seg[1])
            return carry

        lax.fori_loop(0, seg[1] // 2, two, 0)

    def down_dots(idx):
        slots = [lax.rem(j, NPAIR) for j in idx]
        for slot in slots:
            for sub in range(2):
                arrive(slot, sub, FF)
        return [jnp.dot(ab[...], ring[slot, sub, :FF, :], preferred_element_type=F32)
                for slot in slots for sub in range(2)]

    def down(ar, seg):
        first = seg[0]

        def group(n, carry):
            idx = [first + 2 * n, first + 2 * n + 1]
            for k, part in enumerate(down_dots(idx)):
                pb[ar, n * 4 + k] = part
            for j in idx:
                issue(j + NPAIR, first + NPAIR, first + NPAIR + seg[1])
            send1(ar, n).start()

            @pl.when(n >= 1)
            def _():
                stage2(ar, n - 1)

            @pl.when(n >= 2)
            def _():
                stage3(ar, n - 2)

            return carry

        lax.fori_loop(0, 4, group, 0)
        stage2(ar, 3)
        drain(ar)

    def last1(n):
        return pltpu.make_async_remote_copy(
            pb.at[LAST, 2 * n + 1 - c], l1.at[n], b1s, b1r.at[n], device_id=core_peer, device_id_type=MESH_ID)

    def last2(n):
        return pltpu.make_async_remote_copy(
            lsum.at[n], l2.at[n], b2s, b2r.at[n], device_id=y_peer, device_id_type=MESH_ID)

    def own_core(n):
        mine = full.at[s, 2 * n + c]
        return pltpu.make_async_remote_copy(
            mine, mine, os_, or_, device_id=core_peer, device_id_type=MESH_ID)

    def strip(k, n, half):
        src = s if k is None else sp_from[k]
        return full.at[src, 2 * n + c, pl.ds(pl.multiple_of(half * NH, NH), NH)]

    def to_peer(piece, send, recv, peer):
        pltpu.make_async_remote_copy(
            piece, piece, send, recv, device_id=peer, device_id_type=MESH_ID).start()

    def last_stage2(n):
        last1(n).wait_recv()
        lsum[n] = pb[LAST, 2 * n + c] + l1[n]
        last2(n).start()

    def last_stage3(n, whole=False):
        last2(n).wait_recv()
        piece = 2 * n + c
        total = lsum[n] + l2[n]
        for w in range(2):
            cs = slice(w * HD, (w + 1) * HD)
            full[s, piece, :, cs] = round_bf16(hres[piece][:, cs] + gmb[...] * total[:, cs])
        own_core(n).start()
        for k in SP_ORDER:
            mine = full.at[s, piece] if whole else strip(None, n, y)
            to_peer(mine, zss, zrs.at[n], {'sp': sp_peers[k]})

    def z_arrive(n):
        sent(full.at[0, pl.ds(0, 3), pl.ds(0, NH)], zrs.at[n])
        for k in range(3):
            got = strip(k, n, y)
            to_peer(got, yss, yrs.at[n], y_peer)
            to_peer(got, dss, drs, core_peer)

    def y_arrive(n):
        sent(full.at[0, pl.ds(0, 3), pl.ds(0, NH)], yrs.at[n])
        for k in range(3):
            to_peer(strip(k, n, 1 - y), dss, drs, core_peer)

    def whole_arrive(n):
        sent(full.at[0, pl.ds(0, 3)], zrs.at[n])
        for k in range(3):
            to_peer(full.at[sp_from[k], 2 * n + c], dss, drs, core_peer)

    def down_last(seg):
        first = seg[0]

        def group(n, carry):
            for k, part in enumerate(down_dots([first + n])):
                pb[LAST, 2 * n + k] = part
            last1(n).start()

            @pl.when(n >= 1)
            def _():
                last_stage2(n - 1)

            @pl.when(n >= 3)
            def _():
                last_stage3(n - 3)

            return carry

        lax.fori_loop(0, NG, group, 0)
        last_stage2(NG - 1)

    def bytes_of(strips):
        if strips % 2 == 0 and strips <= 2 * NCH:
            return full.at[0, pl.ds(0, strips // 2)]
        return full.at[pl.ds(0, 3), pl.ds(0, strips // 3), pl.ds(0, NH)]

    def spread():
        last_stage3(5)
        z_arrive(0)
        last_stage3(6)
        z_arrive(1)
        last_stage3(7, whole=True)
        for n in range(2, 7):
            z_arrive(n)
            y_arrive(n - 2)
        y_arrive(5)
        whole_arrive(7)
        y_arrive(6)
        own = pl.ds(0, NG)
        for sem in (os_, or_, b1s, b2s):
            sent(full.at[0, own], sem)
        for sem, strips, pieces in ((zss, 21, 3), (yss, 21, 0), (dss, 42, 3), (drs, 42, 3)):
            sent(bytes_of(strips + 2 * pieces), sem)

    def heads_to_rows():
        for h in range(8):
            ofl[:, h * 128:(h + 1) * 128] = osc[pl.ds(h, 16, stride=8), :].astype(BF16)

    hcopy = pltpu.make_async_copy(hid_hbm, hid, hsem)
    hcopy.start()
    xcopy = pltpu.make_async_copy(xv_hbm.at[blk(s, RB)], xvb, xsem)
    xcopy.start()
    barrier = pltpu.get_barrier_semaphore()
    for peer in [core_peer, y_peer] + [{'sp': v} for v in sp_peers]:
        pl.semaphore_signal(barrier, inc=1, device_id=peer, device_id_type=MESH_ID)
    qkv_parts = [cols(wq, j) for j in range(NQ)] + [wk, wv]
    for j, part in enumerate(qkv_parts):
        pltpu.make_async_copy(part, ring.at[j // 2, j % 2], rsem.at[j // 2, j % 2]).start(priority=1)

    def block_of(i):
        return lax.rem(s + 3 - i, NSP)

    def cache_copies(i):
        j = block_of(i)
        return (pltpu.make_async_copy(k_hbm.at[blk(j, RB)], kbuf.at[blk(j, RB)], ksem.at[i]),
                pltpu.make_async_copy(v_hbm.at[blk(j, RB)], vbuf.at[blk(j, RB)], vsem.at[i]))

    for i in range(NSP):
        for cp in cache_copies(i):
            cp.start(priority=1)
    kcopy = pltpu.make_async_copy(kc_hbm.at[blk(s, ROWS)], kbuf, csem.at[0])
    vcopy = pltpu.make_async_copy(vc_hbm.at[blk(s, ROWS)], vbuf, csem.at[1])

    with jax.named_scope('tables'):
        gsc[...] = g1_ref[...].astype(F32)

        def fill(r, carry):
            tab[pl.ds(r, 1), :] = jnp.full((1, HD), pos_ref[r], jnp.int32).astype(F32)
            return carry

        lax.fori_loop(0, ROWS, fill, 0, unroll=8)
        angle = tab[...] * freq_ref[...]
        lanes = lax.broadcasted_iota(jnp.int32, (ROWS, HD), 1)
        sin_v = jnp.sin(angle)
        cosb[...] = jnp.cos(angle)
        sinb[...] = jnp.where(lanes < HD // 2, -sin_v, sin_v)
        for r in range(RB):
            gab[r:r + 1, :] = jnp.full((1, HD), mask_ref[s * RB + r], jnp.int32).astype(F32)
        on = gab[...]
        gab[...] = jnp.tanh(jnp.full((RB, HD), gates_ref[0], F32)) * on
        gmb[...] = jnp.tanh(jnp.full((RB, HD), gates_ref[1], F32)) * on
        xcopy.wait()
        cnt[...] = jnp.broadcast_to(jnp.sum((xvb[...] > 0).astype(jnp.int32), axis=1, keepdims=True), (RB, HD))

    with jax.named_scope('norm'):
        hcopy.wait()

        def norm_rows(r, carry):
            rows = blk(r, RB)
            acc = jnp.zeros((RB, HD), F32)
            for j in range(WIDTH // HD):
                v = hid[rows, j * HD:(j + 1) * HD].astype(F32)
                acc = acc + v * v
            inv = lax.rsqrt(jnp.sum(acc, axis=-1, keepdims=True) * (1.0 / WIDTH) + NORM_EPS)
            for j in range(WIDTH // HD):
                cs = slice(j * HD, (j + 1) * HD)
                x[rows, cs] = (hid[rows, cs].astype(F32) * inv * gsc[j:j + 1, :]).astype(BF16)
            return carry

        lax.fori_loop(0, NSP, norm_rows, 0)

    def rope(part):
        return round_bf16(part * cosb[...] + pltpu.roll(part, HD // 2, 1) * sinb[...])

    def qkv_pair(p):
        for sub in range(2):
            arrive(p, sub, WIDTH)
        return [round_bf16(jnp.dot(x[...], ring[p, sub], preferred_element_type=F32)) for sub in range(2)]

    with jax.named_scope('qkv'):
        def project(p, carry):
            for v, yv in enumerate(qkv_pair(p)):
                for u in range(2):
                    qself[pl.ds(4 * p + 2 * v + u, ROWS, stride=NH), :] = rope(yv[:, u * HD:(u + 1) * HD])
            issue(p + SEG_WO[0], SEG_WO[0], SEG_WO[0] + NQ // 2)
            return carry

        lax.fori_loop(0, NQ // 2, project, 0)
        last_pair = NQ // 2
        for v, yv in enumerate(qkv_pair(last_pair)):
            for u in range(2):
                part = yv[:, u * HD:(u + 1) * HD]
                fresh[pl.ds(2 * v + u, ROWS, stride=NH), :] = part if v else rope(part)
        for p in range(SEG_WO[0] + NQ // 2, SEG_WO[0] + NPAIR):
            issue(p, p, p + 1)

    lane8 = lax.broadcasted_iota(jnp.int32, (NH, HD), 1)
    head8 = lax.broadcasted_iota(jnp.int32, (NH, HD), 0)
    base = s * TBLK

    def part_copy(k):
        peer = lax.rem(s + k + 1, NSP)
        to = {'sp': peer}
        return (pltpu.make_async_remote_copy(o_part.at[blk(peer, HD)], ro.at[k], osem.at[0, k], osem.at[1, k],
                                             device_id=to, device_id_type=MESH_ID),
                pltpu.make_async_remote_copy(stats.at[blk(peer, RB)], rst.at[k], stsem.at[0, k], stsem.at[1, k],
                                             device_id=to, device_id_type=MESH_ID))

    def some_rows(rows):
        lps = [pos_ref[b] - base for b in rows]
        new = [fresh[blk(b, NH), :] for b in rows]
        queries = [qself[blk(b, NH), :].astype(BF16) for b in rows]
        keys = [with_new(kbuf[b], f[0:2], lp) for f, b, lp in zip(new, rows, lps)]
        values = [with_new(vbuf[b], f[2:4], lp) for f, b, lp in zip(new, rows, lps)]
        maxes, sums, outs = attend(queries, keys, values, [lp + 1 for lp in lps], HD ** -0.5)
        for b, m, l, o in zip(rows, maxes, sums, outs):
            o_part[blk(b, NH), :] = o
            st = jnp.where(lane8 == head8, m, 0.0) + jnp.where(lane8 == head8 + NH, l, 0.0)
            stats[pl.ds(b, 1), :] = jnp.sum(st, axis=0, keepdims=True)

    with jax.named_scope('bar'):
        pl.semaphore_wait(barrier, 5)
    with jax.named_scope('attend'):
        def block(i, carry):
            for cp in cache_copies(i):
                cp.wait()

            def some(g, carry2):
                some_rows([block_of(i) * RB + g * UNROLL + u for u in range(UNROLL)])
                return carry2

            lax.fori_loop(0, RB // UNROLL, some, 0)

            @pl.when(i < NSP - 1)
            def _():
                for cp in part_copy(NSP - 2 - i):
                    cp.start()

            return carry

        lax.fori_loop(0, NSP, block, 0)
        kcopy.start(priority=1)
        vcopy.start(priority=1)
    with jax.named_scope('parts'):
        for k in range(3):
            for cp in part_copy(k):
                cp.wait()

    lane3 = lax.broadcasted_iota(jnp.int32, BLK3, 2)
    head3 = lax.broadcasted_iota(jnp.int32, BLK3, 1)

    def pick(st, off):
        return jnp.sum(jnp.where(lane3 == head3 + off, st[:, None, :], 0.0), axis=2, keepdims=True)

    parts = [(o_part[blk(s, HD), :], stats[blk(s, RB), :])]
    parts += [(ro[k], rst[k]) for k in range(3)]
    maxes = [pick(st, 0) for _, st in parts]
    top = jnp.maximum(jnp.maximum(maxes[0], maxes[1]), jnp.maximum(maxes[2], maxes[3]))
    total = jnp.zeros(BLK3, F32)
    denom = jnp.zeros((16, 8, 1), F32)
    for (o, st), m in zip(parts, maxes):
        f = jnp.exp(m - top)
        denom = denom + pick(st, 8) * f
        total = total + o.reshape(BLK3) * f
    osc[...] = (total / denom).reshape(HD, HD)
    heads_to_rows()

    with jax.named_scope('wo'):
        project_out(0, SEG_WO)
    with jax.named_scope('norm2'):
        norm(g2_ref, lambda q: round_bf16(
            hid[blk(s, RB), blk(q, CW)].astype(F32) + tb[0, q]))
    with jax.named_scope('gu'):
        gate_up(SEG_GU)
    with jax.named_scope('dn'):
        down(1, SEG_DN)
    with jax.named_scope('norm3'):
        norm(g3_ref, lambda q: round_bf16(hres[q] + tb[1, q]))

    qn = qn_ref[...].astype(F32)
    first_q = SEG_CQ[0]
    with jax.named_scope('cq'):
        def queries(p, carry):
            slot = lax.rem(first_q + p, NPAIR)
            for sub in range(2):
                arrive(slot, sub, WIDTH)
            both = [jnp.dot(xb[...], ring[slot, sub], preferred_element_type=F32) for sub in range(2)]
            for sub in range(2):
                part = round_bf16(both[sub])
                for u in range(2):
                    v = part[:, u * HD:(u + 1) * HD]
                    inv = lax.rsqrt(jnp.mean(v * v, axis=-1, keepdims=True) + NORM_EPS)
                    qsc[pl.ds(4 * p + 2 * sub + u, RB, stride=NH), :] = round_bf16(v * inv * qn)
            issue(first_q + p + NPAIR, first_q + NPAIR, first_q + NPAIR + 2)
            return carry

        lax.fori_loop(0, 2, queries, 0)

    with jax.named_scope('cross'):
        kcopy.wait()
        vcopy.wait()

        def long_rows(buf, b):
            return buf[pl.ds(b * NSP, NSP)].reshape(NSP * HD, HD)

        def cross_rows(i, carry):
            bs = [i * 4 + u for u in range(4)]
            rows = [blk(b, NH) for b in bs]
            _, sums, outs = attend([qsc[r, :].astype(BF16) for r in rows], [long_rows(kbuf, b) for b in bs], [long_rows(vbuf, b) for b in bs],
                                   [cnt[pl.ds(b, 1), 0:1] for b in bs], HD ** -0.5)
            for r, l, o in zip(rows, sums, outs):
                osc[r, :] = o / l
            return carry

        lax.fori_loop(0, 4, cross_rows, 0)
        heads_to_rows()
    with jax.named_scope('cwo'):
        project_out(2, SEG_CWO)
    with jax.named_scope('norm4'):
        ga = jnp.concatenate([gab[...], gab[...]], axis=1)
        norm(g4_ref, lambda q: round_bf16(hres[q] + ga * tb[2, q]))
    with jax.named_scope('cgu'):
        gate_up(SEG_CGU)
    with jax.named_scope('cdn'):
        down_last(SEG_CDN)
    with jax.named_scope('spread'):
        spread()


def emit_kernel(pos_ref, full_hbm, fresh_hbm, k_hbm, v_hbm, out_hbm, k_out, v_out,
                full, fresh, kbuf, vbuf, out, fsem, nsem, ksem, vsem, kosem, vosem, osem):
    base = lax.axis_index('sp') * TBLK
    ncopy = pltpu.make_async_copy(fresh_hbm, fresh, nsem)
    ncopy.start()

    def copies(j):
        rows = blk(j, RB)
        return ((pltpu.make_async_copy(k_hbm.at[rows], kbuf.at[rows], ksem.at[j]),
                 pltpu.make_async_copy(v_hbm.at[rows], vbuf.at[rows], vsem.at[j])),
                (pltpu.make_async_copy(kbuf.at[rows], k_out.at[rows], kosem.at[j]),
                 pltpu.make_async_copy(vbuf.at[rows], v_out.at[rows], vosem.at[j])))

    for j in range(NSP):
        for cp in copies(j)[0]:
            cp.start()
    fcopy = pltpu.make_async_copy(full_hbm, full, fsem)
    fcopy.start()
    ncopy.wait()
    row_t = lax.broadcasted_iota(jnp.int32, (RB, HD), 0)

    def block(j, carry):
        ins, outs = copies(j)
        for cp in ins:
            cp.wait()

        def some(g, carry2):
            for u in range(UNROLL):
                b = j * RB + g * UNROLL + u
                new = fresh[blk(b, NH), :]
                lp = pos_ref[b] - base
                first = lax.div(jnp.clip(lp, 0, TBLK - 1), NH) * RB
                window = pl.ds(pl.multiple_of(first, RB), RB)
                for buf, pair in ((kbuf, new[0:2]), (vbuf, new[2:4])):
                    both = jnp.where((row_t & 1) == 0, pair[0:1, :], pair[1:2, :])
                    hit = (row_t >> 1) + lax.div(first, 2) == lp
                    buf[b, window, :] = jnp.where(hit, both, buf[b, window, :].astype(F32)).astype(BF16)
            return carry2

        lax.fori_loop(0, RB // UNROLL, some, 0)
        for cp in outs:
            cp.start()
        return carry

    lax.fori_loop(0, NSP, block, 0)
    fcopy.wait()

    def emit(q, carry):
        for r in range(NSP):
            out[r * RB:(r + 1) * RB, blk(q, CW)] = full[r, q].astype(BF16)
        return carry

    lax.fori_loop(0, NCH, emit, 0, unroll=4)
    ocopy = pltpu.make_async_copy(out, out_hbm, osem)
    ocopy.start()
    for j in range(NSP):
        for cp in copies(j)[1]:
            cp.wait()
    ocopy.wait()


def solution(mesh):
    cache_spec = P('dp', 'sp', 'tp', None)
    cross_spec = P('dp', None, 'tp', None)
    row_spec = P('dp', None)
    vec_spec = P('dp')
    full_spec = P(None)
    col_spec = P(None, 'tp')
    split_rows = P('tp', None)
    in_specs = (row_spec, vec_spec, cache_spec, cache_spec, cross_spec, cross_spec, row_spec, vec_spec,
                full_spec, col_spec, col_spec, col_spec, split_rows, full_spec, col_spec, col_spec, split_rows,
                full_spec, col_spec, full_spec, split_rows, full_spec, full_spec, col_spec, col_spec, split_rows)
    out_specs = (row_spec, cache_spec, cache_spec)
    vmem = pl.BlockSpec(memory_space=pltpu.VMEM)
    smem = pl.BlockSpec(memory_space=pltpu.SMEM)
    hbm = pl.BlockSpec(memory_space=pl.ANY)
    dma = pltpu.SemaphoreType.DMA

    def local_step(hidden, new_pos, k_self, v_self, k_cross, v_cross, xvalid, rowmask,
                   self_attn_norm, self_wq, self_wk, self_wv, self_wo, self_mlp_norm,
                   self_wgate, self_wup, self_wdown, cross_attn_norm, cross_wq, cross_qnorm,
                   cross_wo, cross_gates, cross_mlp_norm, cross_wgate, cross_wup, cross_wdown):
        half = rope_freqs(HD)
        freq = np.concatenate([half, half]).reshape(1, HD).astype(np.float32)

        def fold(gain):
            return gain.reshape(WIDTH // HD, HD)

        caches = [cache.reshape(ROWS, HD, HD) for cache in (k_self, v_self)]
        block_row = pltpu.VMEM((RB, HD), F32)
        table = pltpu.VMEM((ROWS, HD), F32)
        heads = pltpu.VMEM((ROWS * NH, HD), F32)
        cache_buf = pltpu.VMEM((ROWS, HD, HD), BF16)
        rows, fresh = pl.pallas_call(
            step_kernel,
            out_shape=(jax.ShapeDtypeStruct((NSP, NCH, RB, CW), F32), jax.ShapeDtypeStruct((ROWS * NH, HD), F32)),
            in_specs=[smem] * 3 + [hbm] * 2 + [vmem] * 6 + [hbm] * 16,
            out_specs=(vmem, vmem),
            scratch_shapes=[
                pltpu.VMEM((NPAIR, 2, WIDTH, CW), BF16),
                cache_buf, cache_buf,
                *[pltpu.VMEM((ROWS, WIDTH), BF16)] * 2, table, table, table, heads, heads, table,
                pltpu.VMEM((RB, 256), jnp.int32), pltpu.VMEM((RB, HD), jnp.int32), block_row, block_row,
                pltpu.VMEM((WIDTH // HD, HD), F32), pltpu.VMEM((NCH, RB, CW), F32),
                pltpu.VMEM((RB, WIDTH), BF16), pltpu.VMEM((RB, FF), BF16), pltpu.VMEM((RB, QW), BF16),
                *[pltpu.VMEM((HD, HD), F32)] * 2, pltpu.VMEM((3, HD, HD), F32), pltpu.VMEM((3, RB, HD), F32),
                pltpu.VMEM((4, NCH, RB, CW), F32), *[pltpu.VMEM((3, 4, 2, RB, CW), F32)] * 3,
                pltpu.VMEM((3, NCH, RB, CW), F32), *[pltpu.VMEM((NG, RB, CW), F32)] * 3,
                dma((NPAIR, 2)), dma((2,)), dma, dma, *[dma((NSP,))] * 2, *[dma((2, 3))] * 2, dma, dma((4,)), dma, dma((2, 4)), dma, dma((4,)),
                *[dma, dma((NG,))] * 2, dma, dma, *[dma, dma((NG,))] * 2, dma, dma],
            compiler_params=pltpu.CompilerParams(
                collective_id=0, has_side_effects=True, vmem_limit_bytes=VMEM_ALL),
            name='step',
        )(new_pos, rowmask, cross_gates, hidden, xvalid, fold(self_attn_norm), fold(self_mlp_norm),
          fold(cross_attn_norm), fold(cross_mlp_norm), cross_qnorm.reshape(1, -1), jnp.asarray(freq), *caches,
          self_wq, self_wk, self_wv, self_wo, self_wgate, self_wup, self_wdown,
          cross_wq, cross_wo, cross_wgate, cross_wup, cross_wdown,
          *[cache.reshape(-1, HD, HD) for cache in (k_cross, v_cross)])
        out, k_new, v_new = pl.pallas_call(
            emit_kernel,
            out_shape=(jax.ShapeDtypeStruct((ROWS, WIDTH), BF16), *[jax.ShapeDtypeStruct((ROWS, HD, HD), BF16)] * 2),
            in_specs=[smem] + [hbm] * 4, out_specs=(hbm,) * 3,
            scratch_shapes=[pltpu.VMEM((NSP, NCH, RB, CW), F32), heads, cache_buf, cache_buf,
                            pltpu.VMEM((ROWS, WIDTH), BF16), dma, dma, *[dma((NSP,))] * 4, dma],
            compiler_params=pltpu.CompilerParams(vmem_limit_bytes=VMEM_ALL),
            name='emit',
        )(new_pos, rows, fresh, *caches)
        return out, k_new.reshape(k_self.shape), v_new.reshape(v_self.shape)

    return jax.shard_map(local_step, mesh=mesh, in_specs=in_specs, out_specs=out_specs, check_vma=False)
```
